32 devices in a mesh: gx: 2 (over y), gy: 4 (over x, core), gz: 4 (over z).
Axes of the slice: x: 2, y: 2, z: 4, core: 2. Of those that a mesh axis runs over, the one named last changes fastest.
Arguments:
- velocity: float32 [32, 64, 3, 512], P('gx', 'gy', None, 'gz'), may hold values from -6 to 6
- marker_pos: float32 [2048, 3, 256], P(('gx', 'gy', 'gz')), may hold values from -130 to 256
- marker_force: float32 [2048, 3, 256], P(('gx', 'gy', 'gz')), may hold values from -6 to 6
- intersect: int32 [2048, 27], P(('gx', 'gy', 'gz')), may hold values from 0 to 1, as said below
- tiles: int32 [2048, 27, 16], P(('gx', 'gy', 'gz')), may hold values from 0 to 255, as said below
Outputs:
- velocity_out: float32 [32, 64, 3, 512], P('gx', 'gy', None, 'gz')
- marker_velocity: float32 [2048, 3, 256], P(('gx', 'gy', 'gz'))
The draws below stay inside these ranges and needn't reach their ends.
Inputs may be any that keep to these rules, and one draw needn't show every extreme that they name: `intersect`: column 13 is always 1. Of one owner's bubbles at most 16 have a 1 in any other column; on every draw some owner has exactly 16 in some column, and some device is intersected by exactly 16 bubbles of its neighbour at each of the 26 other offsets. tiles[b, q, j] is a tile of the device at offset q from b's owner, numbered ix * 16 + iy for the line of cells (ix, iy); entries of columns where intersect is 0 are not used.
All inputs are finite; a program needn't handle non-finite values.
Results may differ from the reference program's by a relative error of at most 0.0049.
Values sent between devices are 32-bit elements; how exact they have to be, the bound alone decides.
A program may use at most 128 MiB of HBM per device.

```python
import math
import jax
import jax.numpy as jnp
import numpy as np
from jax import lax

CX = 16
CY = 16
TILE_LEN = 128
MARKERS = 256
BUB_DEV = 64
CAP = 16
TOUCH = 16
BUBBLES = 2048
NX = 32
NY = 64
NZ = 512
N_GX = 2
N_GY = 4
N_GZ = 4
DEVICES = 32


def direction_offsets():
    direction = jnp.arange(27, dtype=jnp.int32)
    return (direction // 9 - 1, direction // 3 % 3 - 1, direction % 3 - 1)


def intersect_table(key):
    base_key = jax.random.fold_in(key, 7001)
    key_heavy, key_pick, key_count, key_score = jax.random.split(base_key, 4)
    device = jnp.arange(DEVICES, dtype=jnp.int32)
    heavy_recv = (jax.random.randint(key_heavy, (DEVICES,), 0, 4) == 0) | (device == jax.random.randint(key_pick, (), 0, DEVICES))
    light_counts = jax.random.randint(key_count, (DEVICES, 27), 1, max(CAP // 2, 1) + 1)
    recv_counts = jnp.where(heavy_recv[:, None], CAP, light_counts)
    off_x, off_y, off_z = direction_offsets()
    dev_x = device // (N_GY * N_GZ)
    dev_y = device // N_GZ % N_GY
    dev_z = device % N_GZ
    recv_x = (dev_x[:, None] + off_x[None, :]) % N_GX
    recv_y = (dev_y[:, None] + off_y[None, :]) % N_GY
    recv_z = (dev_z[:, None] + off_z[None, :]) % N_GZ
    receiver = (recv_x * N_GY + recv_y) * N_GZ + recv_z
    send_counts = recv_counts[receiver, jnp.arange(27, dtype=jnp.int32)[None, :]]
    scores = jax.random.randint(key_score, (DEVICES, 27, BUB_DEV), 0, 1 << 20) * BUB_DEV + jnp.arange(BUB_DEV, dtype=jnp.int32)
    ranking = jnp.sum((scores[:, :, None, :] < scores[:, :, :, None]).astype(jnp.int32), axis=3)
    chosen = (ranking < send_counts[:, :, None]) | (jnp.arange(27, dtype=jnp.int32)[None, :, None] == 13)
    return jnp.transpose(chosen, (0, 2, 1)).reshape(BUBBLES, 27).astype(jnp.int32)


def tile_table(key):
    base_key = jax.random.fold_in(key, 7002)
    key_cx, key_cy, key_cells = jax.random.split(base_key, 3)
    side = math.isqrt(max(TOUCH - 1, 0)) + 1
    window = min(CX, CY, 2 * side)
    corner_x = jax.random.randint(key_cx, (BUBBLES, 27, 1), 0, CX - window + 1)
    corner_y = jax.random.randint(key_cy, (BUBBLES, 27, 1), 0, CY - window + 1)
    scores = jax.random.randint(key_cells, (BUBBLES, 27, window * window), 0, 1 << 20) * (window * window) + jnp.arange(window * window, dtype=jnp.int32)
    _, cells = lax.top_k(scores, TOUCH)
    cells = cells.astype(jnp.int32)
    return ((corner_x + cells // window) * CY + corner_y + cells % window).astype(jnp.int32)


def draw_intersect(key, part):
    return intersect_table(key)


def draw_tiles(key, part):
    return tile_table(key)


def draw_marker_pos(key, part):
    tile_ids = tile_table(key)
    flags = intersect_table(key)
    anchor_key = jax.random.fold_in(key, 7004)
    key_code, key_slot = jax.random.split(anchor_key, 2)
    count = jnp.sum(flags, axis=1)
    pick = jax.random.randint(key_code, (BUBBLES, MARKERS), 0, count[:, None])
    running = jnp.cumsum(flags, axis=1)
    anchor_dir = jnp.zeros((BUBBLES, MARKERS), jnp.int32)
    for code in range(27):
        anchor_dir = anchor_dir + (running[:, code, None] <= pick).astype(jnp.int32)
    anchor_slot = jax.random.randint(key_slot, (BUBBLES, MARKERS), 0, TOUCH)
    flat_tiles = tile_ids.reshape(BUBBLES, 27 * TOUCH)
    anchored = jnp.take_along_axis(flat_tiles, anchor_dir * TOUCH + anchor_slot, axis=1)
    off_x, off_y, off_z = direction_offsets()
    jitter_key = jax.random.fold_in(key, 7003)
    key_x, key_y, key_z = jax.random.split(jitter_key, 3)
    jitter_width = 1.5
    shape_one = (BUBBLES, MARKERS)
    pos_x = (off_x[anchor_dir] * CX + anchored // CY).astype(jnp.float32) + jax.random.uniform(key_x, shape_one, jnp.float32, -jitter_width, jitter_width)
    pos_y = (off_y[anchor_dir] * CY + anchored % CY).astype(jnp.float32) + jax.random.uniform(key_y, shape_one, jnp.float32, -jitter_width, jitter_width)
    pos_z = (off_z[anchor_dir] * TILE_LEN).astype(jnp.float32) + jax.random.uniform(key_z, shape_one, jnp.float32, 0.0, float(TILE_LEN))
    return jnp.stack([pos_x, pos_y, pos_z], axis=1)


def steps_of(stream_key, extent, cuts, least, top_value):
    def one(dim, blocks):
        steps = jax.random.uniform(jax.random.fold_in(jax.random.fold_in(stream_key, 6), dim), (blocks,), jnp.float32, least / len(cuts), top_value / len(cuts))
        return jnp.repeat(jnp.exp(steps), extent[dim] // blocks).reshape((-1,) + (1,) * (len(extent) - dim - 1))

    factor_of = one(*cuts[0])
    for cut in cuts[1:]:
        factor_of = factor_of * one(*cut)
    return factor_of


def scatter_about(rng, shape, scale, most, cuts=(), kind=jnp.bfloat16):
    result = scale * jax.random.normal(rng, shape, jnp.float32)
    if cuts:
        result = result * steps_of(rng, shape, cuts, -0.22, 0.18)
    return jnp.clip(result, -most, most).astype(kind)


def setup_inputs(seed: int = 0) -> dict:
    key_of = jax.random.split(jax.random.key(seed), 6)
    return {
        "velocity": scatter_about(key_of[0], (NX, NY, 3, NZ), 1.0, 6.0, ((0, 2), (1, 4), (3, 4)), jnp.float32),
        "marker_pos": draw_marker_pos(jax.random.fold_in(key_of[5], 71), 0),
        "marker_force": scatter_about(key_of[2], (BUBBLES, 3, MARKERS), 1.0, 6.0, ((0, 32),), jnp.float32),
        "intersect": draw_intersect(jax.random.fold_in(key_of[5], 71), 0),
        "tiles": draw_tiles(jax.random.fold_in(key_of[5], 71), 0),
    }


spread_width = 0.5
viscous = 0.1


def offset_table():
    direction = jnp.arange(27, dtype=jnp.int32)
    return jnp.stack([direction // 9 - 1, (direction // 3) % 3 - 1, direction % 3 - 1], axis=1)


def line_weights(rel_pos, tile_ids, size_y, tile_len):
    cell_z = jnp.arange(tile_len, dtype=jnp.int32).astype(jnp.float32)
    along_z = jnp.exp(-spread_width * jnp.square(cell_z[None, :, None] - rel_pos[:, 2, None, :])).astype(jnp.bfloat16)
    tile_x = (tile_ids // size_y).astype(jnp.float32)
    tile_y = (tile_ids % size_y).astype(jnp.float32)
    across = jnp.exp(-spread_width * (jnp.square(tile_x[:, :, None] - rel_pos[:, None, 0, :]) + jnp.square(tile_y[:, :, None] - rel_pos[:, None, 1, :])))
    across = jnp.where(tile_ids[:, :, None] >= 0, across, jnp.zeros_like(across))
    return along_z, across


def compact_all(flag_cols):
    ranking = jnp.cumsum(flag_cols, axis=1) - 1
    slot_ids = jnp.arange(CAP, dtype=jnp.int32)
    matches = (ranking[:, None, :, :] == slot_ids[None, :, None, None]) & (flag_cols[:, None, :, :] == 1)
    bubble = jnp.arange(BUB_DEV, dtype=jnp.int32)
    picked = jnp.sum(jnp.where(matches, bubble[None, None, :, None], 0), axis=2).astype(jnp.int32)
    return picked, jnp.any(matches, axis=2)


def receiver_rows(device, marker_pos, marker_force, tiles, picked, usable):
    others = jnp.asarray(np.concatenate([np.arange(13), np.arange(14, 27)]), dtype=jnp.int32)
    offsets = offset_table()[others]
    here_at = jnp.stack([device // (N_GY * N_GZ), (device // N_GZ) % N_GY, device % N_GZ])
    mesh_sizes = jnp.array([N_GX, N_GY, N_GZ], dtype=jnp.int32)
    owner_at = (here_at[None, :] - offsets) % mesh_sizes[None, :]
    owners = ((owner_at[:, 0] * N_GY + owner_at[:, 1]) * N_GZ + owner_at[:, 2]).astype(jnp.int32)
    slot_ids = jnp.arange(CAP, dtype=jnp.int32)
    chosen = picked[owners[:, None], slot_ids[None, :], others[:, None]]
    is_valid = usable[owners[:, None], slot_ids[None, :], others[:, None]]
    global_id = (owners[:, None] * BUB_DEV + chosen).astype(jnp.int32)
    block_size = jnp.array([CX, CY, TILE_LEN], dtype=jnp.float32)
    shifts = offsets.astype(jnp.float32) * block_size[None, :]
    near_pos = marker_pos[global_id] - shifts[:, None, :, None]
    near_force = marker_force[global_id]
    near_tiles = jnp.where(is_valid[:, :, None], tiles[global_id, others[:, None]], -1)
    start = (device * BUB_DEV).astype(jnp.int32)
    own_pos = lax.dynamic_slice_in_dim(marker_pos, start, BUB_DEV, 0)
    own_force = lax.dynamic_slice_in_dim(marker_force, start, BUB_DEV, 0)
    own_tiles = lax.dynamic_slice_in_dim(tiles[:, 13, :], start, BUB_DEV, 0)
    rel_pos = jnp.concatenate([own_pos, near_pos.reshape(-1, 3, MARKERS)], axis=0)
    forces = jnp.concatenate([own_force, near_force.reshape(-1, 3, MARKERS)], axis=0)
    tile_ids = jnp.concatenate([own_tiles, near_tiles.reshape(-1, TOUCH)], axis=0).astype(jnp.int32)
    row_id = jnp.concatenate([start + jnp.arange(BUB_DEV, dtype=jnp.int32), global_id.reshape(-1)], axis=0).astype(jnp.int32)
    row_ok = jnp.concatenate([jnp.ones((BUB_DEV,), dtype=bool), is_valid.reshape(-1)], axis=0)
    return rel_pos, forces, tile_ids, row_id, row_ok


def reference(velocity, marker_pos, marker_force, intersect, tiles):
    flag_cols = intersect.reshape(DEVICES, BUB_DEV, 27)
    picked, usable = compact_all(flag_cols)
    usable = usable & (jnp.arange(27, dtype=jnp.int32)[None, None, :] != 13)
    tile_total = CX * CY

    def spread_one(device):
        rel_pos, forces, tile_ids, row_id, row_ok = receiver_rows(device, marker_pos, marker_force, tiles, picked, usable)
        along_z, across = line_weights(rel_pos, tile_ids, CY, TILE_LEN)
        scaled = (forces[:, None, :, :] * across[:, :, None, :]).astype(jnp.bfloat16)
        pieces = jnp.einsum("rtkm,rcm->rtkc", scaled.astype(jnp.float32), along_z.astype(jnp.float32), precision=lax.Precision.HIGHEST)
        target = jnp.where(tile_ids >= 0, tile_ids, tile_total).reshape(-1)
        summed = jax.ops.segment_sum(pieces.reshape(-1, 3, TILE_LEN), target, num_segments=tile_total + 1)
        return summed[:tile_total]

    forces_all = lax.map(spread_one, jnp.arange(DEVICES, dtype=jnp.int32))
    force_grid = forces_all.reshape(N_GX, N_GY, N_GZ, CX, CY, 3, TILE_LEN).transpose(0, 3, 1, 4, 5, 2, 6).reshape(CX * N_GX, CY * N_GY, 3, TILE_LEN * N_GZ)
    laplace = (jnp.roll(velocity, 1, 0) + jnp.roll(velocity, -1, 0) + jnp.roll(velocity, 1, 1) + jnp.roll(velocity, -1, 1)
               + jnp.roll(velocity, 1, 3) + jnp.roll(velocity, -1, 3) - 6.0 * velocity)
    velocity_out = velocity + viscous * laplace + force_grid
    grid_blocks = velocity_out.reshape(N_GX, CX, N_GY, CY, 3, N_GZ, TILE_LEN).transpose(0, 2, 5, 1, 3, 4, 6).reshape(DEVICES, tile_total, 3, TILE_LEN)

    def sample_one(running, device):
        rel_pos, forces, tile_ids, row_id, row_ok = receiver_rows(device, marker_pos, marker_force, tiles, picked, usable)
        along_z, across = line_weights(rel_pos, tile_ids, CY, TILE_LEN)
        grid_tiles = lax.dynamic_index_in_dim(grid_blocks, device, 0, keepdims=False)
        local_u = jnp.take(grid_tiles, jnp.maximum(tile_ids, 0), axis=0).astype(jnp.bfloat16)
        sampled = jnp.einsum("rtkc,rcm->rtkm", local_u.astype(jnp.float32), along_z.astype(jnp.float32), precision=lax.Precision.HIGHEST)
        partial_value = jnp.sum(sampled * across[:, :, None, :], axis=1)
        partial_value = jnp.where(row_ok[:, None, None], partial_value, jnp.zeros_like(partial_value))
        return running.at[row_id].add(partial_value), None

    marker_velocity, _ = lax.scan(sample_one, jnp.zeros((DEVICES * BUB_DEV, 3, MARKERS), jnp.float32), jnp.arange(DEVICES, dtype=jnp.int32))
    return velocity_out, marker_velocity
```

```python
import functools

import jax
import jax.numpy as jnp
import numpy as np
from jax import lax
from jax.experimental import pallas as pl
from jax.experimental.pallas import tpu as pltpu
from jax.sharding import PartitionSpec as P

CAP = 16
GROUP = 4

spread_width = 0.5
viscous = 0.1
scale = float(np.sqrt(spread_width * np.log2(np.e)))

VMEM = pl.BlockSpec(memory_space=pltpu.VMEM)
SMEM = pl.BlockSpec(memory_space=pltpu.SMEM)


def shifted(value, axis, step):
    count = lax.axis_size(axis)
    return lax.ppermute(value, axis, [(i, (i + step) % count) for i in range(count)])


def message(marker_pos, marker_force, intersect, tiles):
    bubbles, _, markers = marker_pos.shape
    touched = tiles.shape[2]
    own_lists = bubbles // CAP
    ranking = jnp.cumsum(intersect, axis=0) - 1
    slot = jnp.arange(CAP, dtype=jnp.int32)
    matches = (ranking.T[:, None, :] == slot[None, :, None]) & (intersect.T[:, None, :] == 1)
    bubble = jnp.arange(bubbles, dtype=jnp.int32)
    picked = jnp.sum(jnp.where(matches, bubble[None, None, :], 0), axis=2)
    counts = jnp.minimum(jnp.sum(intersect, axis=0), CAP)
    used = slot[None, :] < counts[:, None]
    listed = jnp.einsum(
        "qsb,bqj->qsj",
        matches.astype(jnp.bfloat16),
        tiles.astype(jnp.bfloat16),
        preferred_element_type=jnp.float32,
    )
    listed = jnp.where(used[:, :, None], listed, -1.0).reshape(27, CAP * touched)
    own_tiles = tiles[:, 13, :].astype(jnp.float32).reshape(own_lists, CAP * touched)
    listed = jnp.concatenate([listed[:13], own_tiles[:1], listed[14:], own_tiles[1:]], axis=0)
    own_picks = bubble.reshape(own_lists, CAP)
    picks = jnp.concatenate([picked[:13], own_picks[:1], picked[14:], own_picks[1:]], axis=0)
    counts = jnp.concatenate(
        [counts[:13], jnp.full((1,), CAP), counts[14:], jnp.full((own_lists - 1,), CAP)]
    )
    lists = jnp.concatenate([picks.reshape(-1), counts]).astype(jnp.float32)
    lists = jnp.pad(lists, (0, -lists.shape[0] % markers)).reshape(-1, markers)
    packed = jnp.concatenate(
        [
            marker_pos.transpose(1, 0, 2).reshape(-1, markers),
            marker_force.transpose(1, 0, 2).reshape(-1, markers),
            listed,
            lists,
        ],
        axis=0,
    )
    return jnp.pad(packed, ((0, -packed.shape[0] % 8), (0, 0)))


class Sizes:
    def __init__(self, velocity, marker_pos, tiles):
        self.bubbles, _, self.markers = marker_pos.shape
        self.size_x, self.size_y, _, self.tile_len = velocity.shape
        self.touched = tiles.shape[2]
        self.tile_total = self.size_x * self.size_y
        self.width = CAP * self.touched
        assert self.width == self.markers
        self.own_lists = self.bubbles // CAP
        self.n_lists = 26 + self.own_lists
        self.list_row = 6 * self.bubbles + self.n_lists

    def meta(self, blocks):
        rows = -(-(self.n_lists * (CAP + 1)) // self.markers)
        self.meta_len = rows * self.markers
        parts = [b[self.list_row : self.list_row + rows].reshape(-1) for b in blocks]
        return jnp.concatenate(parts).astype(jnp.int32)


def stack_blocks(blocks, data):
    for i, block in enumerate(blocks):
        data[i] = block[...]


def batch_setup(z, tab, meta, data, cols, i):
    src, lst = tab[6 * i], tab[6 * i + 1]
    base = src * z.meta_len
    count = meta[base + z.n_lists * CAP + lst]
    tile_row = data[src, pl.ds(6 * z.bubbles + lst, 1), :]
    tile_x = jnp.floor((tile_row + 0.5) * (1.0 / z.size_y))
    tile_y = tile_row - tile_x * z.size_y
    which = lax.broadcasted_iota(jnp.int32, (8, z.width), 0)
    stacked = jnp.where(
        which == 0, tile_row, jnp.where(which == 1, tile_x * scale, tile_y * scale)
    )
    cols[...] = stacked.T
    shift_x = (tab[6 * i + 3] * z.size_x).astype(jnp.float32)
    shift_y = (tab[6 * i + 4] * z.size_y).astype(jnp.float32)
    shift_z = (tab[6 * i + 5] * z.tile_len).astype(jnp.float32)
    return src, base + lst * CAP, count, tile_row, (shift_x, shift_y, shift_z)


def row_weights(z, data, cols, src, bubble, slot, shifts):
    def coordinate(k):
        return (data[src, pl.ds(k * z.bubbles + bubble, 1), :] - shifts[k]) * scale

    cell = lax.broadcasted_iota(jnp.int32, (z.tile_len, z.markers), 0).astype(jnp.float32) * scale
    dz = cell - coordinate(2)
    along = jnp.exp2(-(dz * dz)).astype(jnp.bfloat16)
    mine = cols[pl.ds(pl.multiple_of(slot * z.touched, z.touched), z.touched), :]
    dx = jnp.broadcast_to(mine[:, 1:2], (z.touched, z.markers)) - coordinate(0)
    dy = jnp.broadcast_to(mine[:, 2:3], (z.touched, z.markers)) - coordinate(1)
    return along, jnp.exp2(-(dx * dx + dy * dy))


def spread_kernel(z, n_blocks, n_init, n_batches, *refs):
    tab, meta = refs[:2]
    blocks = refs[2 : 2 + n_blocks]
    inits = refs[2 + n_blocks : 2 + n_blocks + n_init]
    acc, data, cols, pieces = refs[2 + n_blocks + n_init :]
    stack_blocks(blocks, data)
    if n_init:
        total = inits[0][...]
        for init in inits[1:]:
            total = total + init[...]
        acc[...] = total
    else:
        acc[...] = jnp.zeros_like(acc)
    pieces[...] = jnp.zeros_like(pieces)

    def batch(i, carry):
        src, first, count, tile_row, shifts = batch_setup(z, tab, meta, data, cols, i)
        target = tab[6 * i + 2]

        def group(g, c):
            for r in range(GROUP):
                slot = g * GROUP + r
                bubble = meta[first + slot]
                along, across = row_weights(z, data, cols, src, bubble, slot, shifts)
                scaled = [
                    (data[src, pl.ds((3 + k) * z.bubbles + bubble, 1), :] * across).astype(
                        jnp.bfloat16
                    )
                    for k in range(3)
                ]
                piece = lax.dot_general(
                    jnp.concatenate(scaled, axis=0),
                    along,
                    (((1,), (1,)), ((), ())),
                    preferred_element_type=jnp.float32,
                ).astype(jnp.bfloat16)
                at = pl.ds(pl.multiple_of(slot * z.touched, z.touched), z.touched)
                for k in range(3):
                    pieces[at, k * z.tile_len : (k + 1) * z.tile_len] = piece[
                        k * z.touched : (k + 1) * z.touched
                    ]
            return c

        lax.fori_loop(0, (count + (GROUP - 1)) // GROUP, group, 0)
        tile = lax.broadcasted_iota(jnp.int32, (z.tile_total, z.width), 0).astype(jnp.float32)
        placing = (tile == tile_row).astype(jnp.float32).astype(jnp.bfloat16)
        added = jnp.dot(placing, pieces[...], preferred_element_type=jnp.float32)
        for k in range(3):
            acc[target, k] += added[:, k * z.tile_len : (k + 1) * z.tile_len]
        return carry

    lax.fori_loop(0, n_batches, batch, 0)


def cost(z, n_batches):
    rows = n_batches * CAP
    return pl.CostEstimate(
        flops=rows * 2 * 3 * z.touched * z.markers * z.tile_len * 8,
        bytes_accessed=4 << 20,
        transcendentals=rows * z.markers * z.tile_len,
    )


def spread(z, blocks, batches, n_acc, inits, name):
    table = jnp.asarray(np.array(batches, np.int32).reshape(-1))
    return pl.pallas_call(
        functools.partial(spread_kernel, z, len(blocks), len(inits), len(batches)),
        out_shape=jax.ShapeDtypeStruct((n_acc, 3, z.tile_total, z.tile_len), jnp.float32),
        in_specs=[SMEM, SMEM] + [VMEM] * (len(blocks) + len(inits)),
        out_specs=VMEM,
        scratch_shapes=[
            pltpu.VMEM((len(blocks),) + blocks[0].shape, jnp.float32),
            pltpu.VMEM((z.width, 8), jnp.float32),
            pltpu.VMEM((z.width, 3 * z.tile_len), jnp.bfloat16),
        ],
        cost_estimate=cost(z, len(batches)),
        name=name,
    )(table, z.meta(blocks), *blocks, *inits)


def sample_kernel(z, n_blocks, n_grids, n_init, n_batches, *refs):
    tab, meta = refs[:2]
    at = 2 + n_blocks
    blocks = refs[2:at]
    grids = refs[at : at + n_grids]
    inits = refs[at + n_grids : at + n_grids + n_init]
    outs = refs[at + n_grids + n_init : at + n_grids + n_init + n_blocks]
    data, cols, local, low, acc = refs[at + n_grids + n_init + n_blocks :]
    stack_blocks(blocks, data)
    for i in range(n_blocks):
        acc[i] = inits[i][...] if n_init else jnp.zeros_like(inits[i] if n_init else outs[i])
    for i, grid in enumerate(grids):
        for k in range(3):
            low[i, :, k * z.tile_len : (k + 1) * z.tile_len] = grid[k].astype(jnp.bfloat16)

    def batch(i, carry):
        src, first, count, _, shifts = batch_setup(z, tab, meta, data, cols, i)
        target = tab[6 * i + 2]
        tile = lax.broadcasted_iota(jnp.int32, (z.width, z.tile_total), 1).astype(jnp.float32)
        picking = (jnp.broadcast_to(cols[:, 0:1], tile.shape) == tile).astype(jnp.float32)
        local[...] = jnp.dot(
            picking.astype(jnp.bfloat16), low[target], preferred_element_type=jnp.float32
        ).astype(jnp.bfloat16)

        def group(g, c):
            for r in range(GROUP):
                slot = g * GROUP + r
                bubble = meta[first + slot]
                along, across = row_weights(z, data, cols, src, bubble, slot, shifts)
                rows = local[pl.ds(pl.multiple_of(slot * z.touched, z.touched), z.touched), :]
                u = jnp.concatenate(
                    [rows[:, k * z.tile_len : (k + 1) * z.tile_len] for k in range(3)], axis=0
                )
                sampled = jnp.dot(u, along, preferred_element_type=jnp.float32)
                for k in range(3):
                    part = jnp.sum(
                        sampled[k * z.touched : (k + 1) * z.touched] * across,
                        axis=0,
                        keepdims=True,
                    )
                    acc[src, pl.ds(k * z.bubbles + bubble, 1), :] += part
            return c

        lax.fori_loop(0, (count + (GROUP - 1)) // GROUP, group, 0)
        return carry

    lax.fori_loop(0, n_batches, batch, 0)
    for i in range(n_blocks):
        outs[i][...] = acc[i]


def sample(z, blocks, grids, batches, inits, name):
    table = jnp.asarray(np.array(batches, np.int32).reshape(-1))
    n = len(blocks)
    shape = (3 * z.bubbles, z.markers)
    return pl.pallas_call(
        functools.partial(sample_kernel, z, n, len(grids), len(inits), len(batches)),
        out_shape=[jax.ShapeDtypeStruct(shape, jnp.float32)] * n,
        in_specs=[SMEM, SMEM] + [VMEM] * (n + len(grids) + len(inits)),
        out_specs=[VMEM] * n,
        scratch_shapes=[
            pltpu.VMEM((n,) + blocks[0].shape, jnp.float32),
            pltpu.VMEM((z.width, 8), jnp.float32),
            pltpu.VMEM((z.width, 3 * z.tile_len), jnp.bfloat16),
            pltpu.VMEM((len(grids), z.tile_total, 3 * z.tile_len), jnp.bfloat16),
            pltpu.VMEM((n,) + shape, jnp.float32),
        ],
        cost_estimate=cost(z, len(batches)),
        name=name,
    )(table, z.meta(blocks), *blocks, *grids, *inits)


def smooth_kernel(vel, x_low, x_high, y_low, y_high, out):
    _, size_x, size_y, tile_len = vel.shape
    total = size_x * size_y
    row = lax.broadcasted_iota(jnp.int32, (size_x, size_y, tile_len), 1)
    lane = lax.broadcasted_iota(jnp.int32, (total, tile_len), 1)
    for k in range(3):
        v = vel[k]
        flat = v.reshape(total, tile_len)
        up = jnp.concatenate([x_low[k][None], v[:-1]], axis=0)
        down = jnp.concatenate([v[1:], x_high[k][None]], axis=0)
        left = jnp.where(row == 0, y_low[k][:, None, :], pltpu.roll(v, 1, 1))
        right = jnp.where(row == size_y - 1, y_high[k][:, None, :], pltpu.roll(v, size_y - 1, 1))
        before = pltpu.roll(flat, 1, 1)
        after = pltpu.roll(flat, tile_len - 1, 1)
        near = (up + down + left + right).reshape(total, tile_len)
        near = near + jnp.where(lane == 0, 0.0, before)
        near = near + jnp.where(lane == tile_len - 1, 0.0, after)
        out[0, k] = flat + viscous * (near - 6.0 * flat)
        out[1, k] = jnp.where(lane == tile_len - 1, viscous * after, 0.0)
        out[2, k] = jnp.where(lane == 0, viscous * before, 0.0)


def body(velocity, marker_pos, marker_force, intersect, tiles):
    z = Sizes(velocity, marker_pos, tiles)
    vel = velocity.transpose(2, 0, 1, 3)

    def code(ox, oy, oz):
        return 9 * (ox + 1) + 3 * (oy + 1) + oz + 1

    x_low = shifted(vel[:, -1], "gx", 1)
    x_high = shifted(vel[:, 0], "gx", -1)
    y_low = shifted(vel[:, :, -1], "gy", 1)
    y_high = shifted(vel[:, :, 0], "gy", -1)

    own = message(marker_pos, marker_force, intersect, tiles)
    if lax.axis_size("gx") == 2:
        x_steps = [(1, (1, -1))]
    else:
        x_steps = [(1, (1,)), (-1, (-1,))]
    x_blocks = [shifted(own, "gx", step) for step, _ in x_steps]
    y_blocks = [shifted(own, "gy", step) for step in (1, -1)]
    xy_blocks = [shifted(block, "gy", step) for step in (1, -1) for block in x_blocks]

    order = {0: 0, -1: 1, 1: 2}

    def own_batches(zs, slot_of):
        found = []
        for oz in zs:
            if oz == 0:
                found += [(0, q, slot_of[0], 0, 0, 0) for q in [13] + list(range(27, z.n_lists))]
            else:
                found.append((0, code(0, 0, oz), slot_of[oz], 0, 0, oz))
        return found

    def x_batches(zs, slot_of, base=0):
        return [
            (base + i, code(ox, 0, oz), slot_of[oz], ox, 0, oz)
            for i, (_, oxs) in enumerate(x_steps)
            for ox in oxs
            for oz in zs
        ]

    def y_batches(zs, slot_of, base=0):
        return [
            (base + i, code(0, oy, oz), slot_of[oz], 0, oy, oz)
            for i, oy in enumerate((1, -1))
            for oz in zs
        ]

    def xy_batches(zs, slot_of, base=0):
        return [
            (base + i * len(x_steps) + j, code(ox, oy, oz), slot_of[oz], ox, oy, oz)
            for i, oy in enumerate((1, -1))
            for j, (_, oxs) in enumerate(x_steps)
            for ox in oxs
            for oz in zs
        ]

    every = (-1, 1, 0)
    acc = spread(z, [own], own_batches(every, order), 3, [], "spread_own")
    smooth = pl.pallas_call(
        smooth_kernel,
        out_shape=jax.ShapeDtypeStruct((3, 3, z.tile_total, z.tile_len), jnp.float32),
        in_specs=[VMEM] * 5,
        out_specs=VMEM,
        name="smooth",
    )(vel, x_low, x_high, y_low, y_high)
    mid = y_blocks + x_blocks
    acc = spread(
        z, mid, y_batches((-1, 1), order) + x_batches(every, order, 2), 3, [acc, smooth], "spread_mid"
    )
    acc = spread(z, xy_blocks, xy_batches((-1, 1), order), 3, [acc], "spread_far")
    from_high = shifted(acc[1], "gz", -1)
    from_low = shifted(acc[2], "gz", 1)
    late = y_blocks + xy_blocks
    zero = {0: 0}
    last = spread(
        z, late, y_batches((0,), zero) + xy_batches((0,), zero, 2), 1, [acc[:1]], "spread_late"
    )
    result = last[0] + from_high + from_low
    low_grid = shifted(result, "gz", 1)
    high_grid = shifted(result, "gz", -1)
    velocity_out = result.reshape(3, z.size_x, z.size_y, z.tile_len).transpose(1, 2, 0, 3)

    far = y_blocks + xy_blocks
    near = [own] + x_blocks
    far_part = sample(
        z, far, [result], y_batches((0,), zero) + xy_batches((0,), zero, 2), [], "sample_far"
    )
    near_part = sample(
        z, near, [result], own_batches((0,), zero) + x_batches((0,), zero, 1), [], "sample_near"
    )
    sides = {-1: 0, 1: 1}
    far_part = sample(
        z,
        far,
        [low_grid, high_grid],
        y_batches((-1, 1), sides) + xy_batches((-1, 1), sides, 2),
        far_part,
        "sample_far_z",
    )
    n_x = len(x_steps)
    xy_back = [
        shifted(far_part[2 + i * n_x + j], "gy", -oy) for i, oy in enumerate((1, -1)) for j in range(n_x)
    ]
    y_back = [shifted(far_part[i], "gy", -oy) for i, oy in enumerate((1, -1))]
    near_part = sample(
        z,
        near,
        [low_grid, high_grid],
        own_batches((-1, 1), sides) + x_batches((-1, 1), sides, 1),
        near_part,
        "sample_near_z",
    )
    total = near_part[0]
    for j, (step, _) in enumerate(x_steps):
        side = near_part[1 + j] + xy_back[j] + xy_back[n_x + j]
        total = total + shifted(side, "gx", -step)
    total = total + y_back[0] + y_back[1]
    marker_velocity = total.reshape(3, z.bubbles, z.markers).transpose(1, 0, 2)
    return (velocity_out, marker_velocity)


def solution(mesh):
    rows = P(("gx", "gy", "gz"), None, None)
    grid = P("gx", "gy", None, "gz")
    return jax.shard_map(
        body,
        mesh=mesh,
        in_specs=(grid, rows, rows, P(("gx", "gy", "gz"), None), rows),
        out_specs=(grid, rows),
        check_vma=False,
    )
```

```python
import functools

import jax
import jax.numpy as jnp
import numpy as np
from jax import lax
from jax.experimental import pallas as pl
from jax.experimental.pallas import tpu as pltpu
from jax.sharding import PartitionSpec as P

CAP = 16
GROUP = 4
VMEM_LIMIT = 20 << 20

spread_width = 0.5
viscous = 0.1
scale = float(np.sqrt(spread_width * np.log2(np.e)))

VMEM = pl.BlockSpec(memory_space=pltpu.VMEM)
SMEM = pl.BlockSpec(memory_space=pltpu.SMEM)


def shifted(value, axis, step):
    count = lax.axis_size(axis)
    return lax.ppermute(value, axis, [(i, (i + step) % count) for i in range(count)])


def message(marker_pos, marker_force, intersect, tiles):
    bubbles, _, markers = marker_pos.shape
    touched = tiles.shape[2]
    own_lists = bubbles // CAP
    ranking = jnp.cumsum(intersect, axis=0) - 1
    slot = jnp.arange(CAP, dtype=jnp.int32)
    matches = (ranking.T[:, None, :] == slot[None, :, None]) & (intersect.T[:, None, :] == 1)
    bubble = jnp.arange(bubbles, dtype=jnp.int32)
    picked = jnp.sum(jnp.where(matches, bubble[None, None, :], 0), axis=2)
    counts = jnp.minimum(jnp.sum(intersect, axis=0), CAP)
    used = slot[None, :] < counts[:, None]
    listed = jnp.einsum(
        "qsb,bqj->qsj",
        matches.astype(jnp.bfloat16),
        tiles.astype(jnp.bfloat16),
        preferred_element_type=jnp.float32,
    )
    listed = jnp.where(used[:, :, None], listed, -1.0).reshape(27, CAP * touched)
    own_tiles = tiles[:, 13, :].astype(jnp.float32).reshape(own_lists, CAP * touched)
    listed = jnp.concatenate([listed[:13], own_tiles[:1], listed[14:], own_tiles[1:]], axis=0)
    own_picks = bubble.reshape(own_lists, CAP)
    picks = jnp.concatenate([picked[:13], own_picks[:1], picked[14:], own_picks[1:]], axis=0)
    counts = jnp.concatenate(
        [counts[:13], jnp.full((1,), CAP), counts[14:], jnp.full((own_lists - 1,), CAP)]
    )
    lists = jnp.concatenate([picks.reshape(-1), counts]).astype(jnp.float32)
    lists = jnp.pad(lists, (0, -lists.shape[0] % markers)).reshape(-1, markers)
    packed = jnp.concatenate(
        [
            marker_pos.transpose(1, 0, 2).reshape(-1, markers),
            marker_force.transpose(1, 0, 2).reshape(-1, markers),
            listed,
            lists,
        ],
        axis=0,
    )
    return jnp.pad(packed, ((0, -packed.shape[0] % 8), (0, 0)))


class Sizes:
    def __init__(self, velocity, marker_pos, tiles):
        self.bubbles, _, self.markers = marker_pos.shape
        self.size_x, self.size_y, _, self.tile_len = velocity.shape
        self.touched = tiles.shape[2]
        self.tile_total = self.size_x * self.size_y
        self.width = CAP * self.touched
        assert self.width == self.markers
        self.own_lists = self.bubbles // CAP
        self.n_lists = 26 + self.own_lists
        self.list_row = 6 * self.bubbles + self.n_lists

    def meta(self, blocks):
        rows = -(-(self.n_lists * (CAP + 1)) // self.markers)
        self.meta_len = rows * self.markers
        parts = [b[self.list_row : self.list_row + rows].reshape(-1) for b in blocks]
        return jnp.concatenate(parts).astype(jnp.int32)


def stack_blocks(z, blocks, data, cell):
    cell[...] = lax.broadcasted_iota(jnp.int32, cell.shape, 0).astype(jnp.float32) * scale
    for i, block in enumerate(blocks):
        data[i] = block[...]


def batch_setup(z, tab, meta, meta_at, data, cols, i):
    src, lst = tab[6 * i], tab[6 * i + 1]
    base = (src + meta_at) * z.meta_len
    count = meta[base + z.n_lists * CAP + lst]
    tile_row = data[src, pl.ds(6 * z.bubbles + lst, 1), :]
    tile_x = jnp.floor((tile_row + 0.5) * (1.0 / z.size_y))
    tile_y = tile_row - tile_x * z.size_y
    which = lax.broadcasted_iota(jnp.int32, (8, z.width), 0)
    stacked = jnp.where(
        which == 0, tile_row, jnp.where(which == 1, tile_x * scale, tile_y * scale)
    )
    cols[...] = stacked.T
    shift_x = (tab[6 * i + 3] * z.size_x).astype(jnp.float32)
    shift_y = (tab[6 * i + 4] * z.size_y).astype(jnp.float32)
    shift_z = (tab[6 * i + 5] * z.tile_len).astype(jnp.float32)
    return src, base + lst * CAP, count, tile_row, (shift_x, shift_y, shift_z)


def row_weights(z, data, cols, cell, src, bubble, slot, shifts):
    def coordinate(k):
        return (data[src, pl.ds(k * z.bubbles + bubble, 1), :] - shifts[k]) * scale

    dz = (cell[...] - coordinate(2)).astype(jnp.bfloat16)
    along = jnp.exp2(-(dz * dz))
    mine = cols[pl.ds(pl.multiple_of(slot * z.touched, z.touched), z.touched), :]
    dx = jnp.broadcast_to(mine[:, 1:2], (z.touched, z.markers)) - coordinate(0)
    dy = jnp.broadcast_to(mine[:, 2:3], (z.touched, z.markers)) - coordinate(1)
    return along, jnp.exp2(-(dx * dx + dy * dy))


def spread_kernel(z, n_blocks, n_init, n_batches, meta_at, *refs):
    tab, meta = refs[:2]
    blocks = refs[2 : 2 + n_blocks]
    inits = refs[2 + n_blocks : 2 + n_blocks + n_init]
    acc, data, cols, cell, pieces = refs[2 + n_blocks + n_init :]
    stack_blocks(z, blocks, data, cell)
    if n_init:
        total = inits[0][...]
        for init in inits[1:]:
            total = total + init[...]
        acc[...] = total
    else:
        acc[...] = jnp.zeros_like(acc)
    pieces[...] = jnp.zeros_like(pieces)

    def batch(i, carry):
        src, first, count, tile_row, shifts = batch_setup(z, tab, meta, meta_at, data, cols, i)
        target = tab[6 * i + 2]

        def group(g, c):
            for r in range(GROUP):
                slot = g * GROUP + r
                bubble = meta[first + slot]
                along, across = row_weights(z, data, cols, cell, src, bubble, slot, shifts)
                scaled = [
                    (data[src, pl.ds((3 + k) * z.bubbles + bubble, 1), :] * across).astype(
                        jnp.bfloat16
                    )
                    for k in range(3)
                ]
                piece = lax.dot_general(
                    jnp.concatenate(scaled, axis=0),
                    along,
                    (((1,), (1,)), ((), ())),
                    preferred_element_type=jnp.float32,
                ).astype(jnp.bfloat16)
                at = pl.ds(pl.multiple_of(slot * z.touched, z.touched), z.touched)
                for k in range(3):
                    pieces[at, k * z.tile_len : (k + 1) * z.tile_len] = piece[
                        k * z.touched : (k + 1) * z.touched
                    ]
            return c

        lax.fori_loop(0, (count + (GROUP - 1)) // GROUP, group, 0)
        tile = lax.broadcasted_iota(jnp.int32, (z.tile_total, z.width), 0).astype(jnp.float32)
        placing = (tile == tile_row).astype(jnp.float32).astype(jnp.bfloat16)
        added = jnp.dot(placing, pieces[...], preferred_element_type=jnp.float32)
        for k in range(3):
            acc[target, k] += added[:, k * z.tile_len : (k + 1) * z.tile_len]
        return carry

    lax.fori_loop(0, n_batches, batch, 0)


def cost(z, n_batches):
    rows = n_batches * CAP
    return pl.CostEstimate(
        flops=rows * 2 * 3 * z.touched * z.markers * z.tile_len * 8,
        bytes_accessed=4 << 20,
        transcendentals=rows * z.markers * z.tile_len,
    )


def spread(z, meta, meta_at, blocks, batches, n_acc, inits, name):
    table = jnp.asarray(np.array(batches, np.int32).reshape(-1))
    return pl.pallas_call(
        functools.partial(spread_kernel, z, len(blocks), len(inits), len(batches), meta_at),
        compiler_params=pltpu.CompilerParams(vmem_limit_bytes=VMEM_LIMIT),
        out_shape=jax.ShapeDtypeStruct((n_acc, 3, z.tile_total, z.tile_len), jnp.float32),
        in_specs=[SMEM, SMEM] + [VMEM] * (len(blocks) + len(inits)),
        out_specs=VMEM,
        scratch_shapes=[
            pltpu.VMEM((len(blocks),) + blocks[0].shape, jnp.float32),
            pltpu.VMEM((z.width, 8), jnp.float32),
            pltpu.VMEM((z.tile_len, z.markers), jnp.float32),
            pltpu.VMEM((z.width, 3 * z.tile_len), jnp.bfloat16),
        ],
        cost_estimate=cost(z, len(batches)),
        name=name,
    )(table, meta, *blocks, *inits)


def sample_kernel(z, n_blocks, n_grids, n_init, n_batches, meta_at, *refs):
    tab, meta = refs[:2]
    at = 2 + n_blocks
    blocks = refs[2:at]
    grids = refs[at : at + n_grids]
    inits = refs[at + n_grids : at + n_grids + n_init]
    outs = refs[at + n_grids + n_init : at + n_grids + n_init + n_blocks]
    data, cols, cell, local, low, acc = refs[at + n_grids + n_init + n_blocks :]
    stack_blocks(z, blocks, data, cell)
    for i in range(n_blocks):
        acc[i] = inits[i][...] if n_init else jnp.zeros_like(inits[i] if n_init else outs[i])
    for i, grid in enumerate(grids):
        for k in range(3):
            low[i, :, k * z.tile_len : (k + 1) * z.tile_len] = grid[k].astype(jnp.bfloat16)

    def batch(i, carry):
        src, first, count, _, shifts = batch_setup(z, tab, meta, meta_at, data, cols, i)
        target = tab[6 * i + 2]
        tile = lax.broadcasted_iota(jnp.int32, (z.width, z.tile_total), 1).astype(jnp.float32)
        picking = (jnp.broadcast_to(cols[:, 0:1], tile.shape) == tile).astype(jnp.float32)
        local[...] = jnp.dot(
            picking.astype(jnp.bfloat16), low[target], preferred_element_type=jnp.float32
        ).astype(jnp.bfloat16)

        def group(g, c):
            for r in range(GROUP):
                slot = g * GROUP + r
                bubble = meta[first + slot]
                along, across = row_weights(z, data, cols, cell, src, bubble, slot, shifts)
                rows = local[pl.ds(pl.multiple_of(slot * z.touched, z.touched), z.touched), :]
                u = jnp.concatenate(
                    [rows[:, k * z.tile_len : (k + 1) * z.tile_len] for k in range(3)], axis=0
                )
                sampled = jnp.dot(u, along, preferred_element_type=jnp.float32)
                for k in range(3):
                    part = jnp.sum(
                        sampled[k * z.touched : (k + 1) * z.touched] * across,
                        axis=0,
                        keepdims=True,
                    )
                    acc[src, pl.ds(k * z.bubbles + bubble, 1), :] += part
            return c

        lax.fori_loop(0, (count + (GROUP - 1)) // GROUP, group, 0)
        return carry

    lax.fori_loop(0, n_batches, batch, 0)
    for i in range(n_blocks):
        outs[i][...] = acc[i]


def sample(z, meta, meta_at, blocks, grids, batches, inits, name):
    table = jnp.asarray(np.array(batches, np.int32).reshape(-1))
    n = len(blocks)
    shape = (3 * z.bubbles, z.markers)
    return pl.pallas_call(
        functools.partial(sample_kernel, z, n, len(grids), len(inits), len(batches), meta_at),
        compiler_params=pltpu.CompilerParams(vmem_limit_bytes=VMEM_LIMIT),
        out_shape=[jax.ShapeDtypeStruct(shape, jnp.float32)] * n,
        in_specs=[SMEM, SMEM] + [VMEM] * (n + len(grids) + len(inits)),
        out_specs=[VMEM] * n,
        scratch_shapes=[
            pltpu.VMEM((n,) + blocks[0].shape, jnp.float32),
            pltpu.VMEM((z.width, 8), jnp.float32),
            pltpu.VMEM((z.tile_len, z.markers), jnp.float32),
            pltpu.VMEM((z.width, 3 * z.tile_len), jnp.bfloat16),
            pltpu.VMEM((len(grids), z.tile_total, 3 * z.tile_len), jnp.bfloat16),
            pltpu.VMEM((n,) + shape, jnp.float32),
        ],
        cost_estimate=cost(z, len(batches)),
        name=name,
    )(table, meta, *blocks, *grids, *inits)


def smooth_kernel(vel, x_low, x_high, y_low, y_high, out):
    _, size_x, size_y, tile_len = vel.shape
    total = size_x * size_y
    row = lax.broadcasted_iota(jnp.int32, (size_x, size_y, tile_len), 1)
    lane = lax.broadcasted_iota(jnp.int32, (total, tile_len), 1)
    for k in range(3):
        v = vel[k]
        flat = v.reshape(total, tile_len)
        up = jnp.concatenate([x_low[k][None], v[:-1]], axis=0)
        down = jnp.concatenate([v[1:], x_high[k][None]], axis=0)
        left = jnp.where(row == 0, y_low[k][:, None, :], pltpu.roll(v, 1, 1))
        right = jnp.where(row == size_y - 1, y_high[k][:, None, :], pltpu.roll(v, size_y - 1, 1))
        before = pltpu.roll(flat, 1, 1)
        after = pltpu.roll(flat, tile_len - 1, 1)
        near = (up + down + left + right).reshape(total, tile_len)
        near = near + jnp.where(lane == 0, 0.0, before)
        near = near + jnp.where(lane == tile_len - 1, 0.0, after)
        out[0, k] = flat + viscous * (near - 6.0 * flat)
        out[1, k] = jnp.where(lane == tile_len - 1, viscous * after, 0.0)
        out[2, k] = jnp.where(lane == 0, viscous * before, 0.0)


def body(velocity, marker_pos, marker_force, intersect, tiles):
    z = Sizes(velocity, marker_pos, tiles)
    vel = velocity.transpose(2, 0, 1, 3)

    def code(ox, oy, oz):
        return 9 * (ox + 1) + 3 * (oy + 1) + oz + 1

    x_low = shifted(vel[:, -1], "gx", 1)
    x_high = shifted(vel[:, 0], "gx", -1)
    y_low = shifted(vel[:, :, -1], "gy", 1)
    y_high = shifted(vel[:, :, 0], "gy", -1)

    own = message(marker_pos, marker_force, intersect, tiles)
    own, x_low, x_high, y_low, y_high = lax.optimization_barrier(
        (own, x_low, x_high, y_low, y_high)
    )
    if lax.axis_size("gx") == 2:
        x_steps = [(1, (1, -1))]
    else:
        x_steps = [(1, (1,)), (-1, (-1,))]
    x_blocks = [shifted(own, "gx", step) for step, _ in x_steps]
    y_blocks = [shifted(own, "gy", step) for step in (1, -1)]
    xy_blocks = [shifted(block, "gy", step) for step in (1, -1) for block in x_blocks]

    order = {0: 0, -1: 1, 1: 2}

    def own_batches(zs, slot_of):
        found = []
        for oz in zs:
            if oz == 0:
                found += [(0, q, slot_of[0], 0, 0, 0) for q in [13] + list(range(27, z.n_lists))]
            else:
                found.append((0, code(0, 0, oz), slot_of[oz], 0, 0, oz))
        return found

    def x_batches(zs, slot_of, base=0):
        return [
            (base + i, code(ox, 0, oz), slot_of[oz], ox, 0, oz)
            for i, (_, oxs) in enumerate(x_steps)
            for ox in oxs
            for oz in zs
        ]

    def y_batches(zs, slot_of, base=0):
        return [
            (base + i, code(0, oy, oz), slot_of[oz], 0, oy, oz)
            for i, oy in enumerate((1, -1))
            for oz in zs
        ]

    def xy_batches(zs, slot_of, base=0):
        return [
            (base + i * len(x_steps) + j, code(ox, oy, oz), slot_of[oz], ox, oy, oz)
            for i, oy in enumerate((1, -1))
            for j, (_, oxs) in enumerate(x_steps)
            for ox in oxs
            for oz in zs
        ]

    n_x = len(x_steps)
    every, outer, zero, sides = (-1, 1, 0), (-1, 1), {0: 0}, {-1: 0, 1: 1}
    metas = [z.meta([own])]
    acc = spread(z, metas[0], 0, [own], own_batches(every, order), 3, [], "spread_own")
    smooth = pl.pallas_call(
        smooth_kernel,
        out_shape=jax.ShapeDtypeStruct((3, 3, z.tile_total, z.tile_len), jnp.float32),
        in_specs=[VMEM] * 5,
        out_specs=VMEM,
        compiler_params=pltpu.CompilerParams(vmem_limit_bytes=VMEM_LIMIT),
        name="smooth",
    )(vel, x_low, x_high, y_low, y_high)
    mid = x_blocks + y_blocks
    metas.append(z.meta(mid))
    acc = spread(
        z,
        metas[1],
        0,
        mid,
        x_batches(outer, order) + y_batches(outer, order, n_x),
        3,
        [acc, smooth],
        "spread_mid",
    )
    metas.append(z.meta(xy_blocks))
    acc = spread(
        z, metas[2], 0, xy_blocks, xy_batches(outer, order), 3, [acc], "spread_far"
    )
    from_high = shifted(acc[1], "gz", -1)
    from_low = shifted(acc[2], "gz", 1)
    near = [own] + x_blocks
    far = y_blocks + xy_blocks
    meta = jnp.concatenate(metas)
    late = x_batches((0,), zero) + y_batches((0,), zero, n_x) + xy_batches((0,), zero, n_x + 2)
    last = spread(z, meta, 1, x_blocks + far, late, 1, [acc[:1]], "spread_late")
    result = last[0] + from_high + from_low
    low_grid = shifted(result, "gz", 1)
    high_grid = shifted(result, "gz", -1)
    velocity_out = result.reshape(3, z.size_x, z.size_y, z.tile_len).transpose(1, 2, 0, 3)

    here = (
        own_batches((0,), zero)
        + x_batches((0,), zero, 1)
        + y_batches((0,), zero, 1 + n_x)
        + xy_batches((0,), zero, 3 + n_x)
    )
    part = sample(z, meta, 0, near + far, [result], here, [], "sample_here")
    far_part = sample(
        z,
        meta,
        1 + n_x,
        far,
        [low_grid, high_grid],
        y_batches(outer, sides) + xy_batches(outer, sides, 2),
        part[1 + n_x :],
        "sample_far",
    )
    xy_back = [
        shifted(far_part[2 + i * n_x + j], "gy", -oy) for i, oy in enumerate((1, -1)) for j in range(n_x)
    ]
    y_back = [shifted(far_part[i], "gy", -oy) for i, oy in enumerate((1, -1))]
    near_part = sample(
        z,
        meta,
        0,
        near,
        [low_grid, high_grid],
        own_batches(outer, sides) + x_batches(outer, sides, 1),
        part[: 1 + n_x],
        "sample_near",
    )
    total = near_part[0]
    for j, (step, _) in enumerate(x_steps):
        side = near_part[1 + j] + xy_back[j] + xy_back[n_x + j]
        total = total + shifted(side, "gx", -step)
    total = total + y_back[0] + y_back[1]
    marker_velocity = total.reshape(3, z.bubbles, z.markers).transpose(1, 0, 2)
    return (velocity_out, marker_velocity)


def solution(mesh):
    rows = P(("gx", "gy", "gz"), None, None)
    grid = P("gx", "gy", None, "gz")
    return jax.shard_map(
        body,
        mesh=mesh,
        in_specs=(grid, rows, rows, P(("gx", "gy", "gz"), None), rows),
        out_specs=(grid, rows),
        check_vma=False,
    )
```

```python
import functools

import jax
import jax.numpy as jnp
import numpy as np
from jax import lax
from jax.experimental import pallas as pl
from jax.experimental.pallas import tpu as pltpu
from jax.sharding import PartitionSpec as P

CAP = 16
STEPS = (CAP // 4, CAP // 2, CAP)
VMEM_LIMIT = 20 << 20

spread_width = 0.5
viscous = 0.1
scale = float(np.sqrt(spread_width * np.log2(np.e)))

VMEM = pl.BlockSpec(memory_space=pltpu.VMEM)
SMEM = pl.BlockSpec(memory_space=pltpu.SMEM)


def shifted(value, axis, step):
    count = lax.axis_size(axis)
    return lax.ppermute(value, axis, [(i, (i + step) % count) for i in range(count)])


def message(marker_pos, marker_force, intersect, tiles):
    bubbles, _, markers = marker_pos.shape
    touched = tiles.shape[2]
    own_lists = bubbles // CAP
    ranking = jnp.cumsum(intersect, axis=0) - 1
    slot = jnp.arange(CAP, dtype=jnp.int32)
    matches = (ranking.T[:, None, :] == slot[None, :, None]) & (intersect.T[:, None, :] == 1)
    bubble = jnp.arange(bubbles, dtype=jnp.int32)
    picked = jnp.sum(jnp.where(matches, bubble[None, None, :], 0), axis=2)
    counts = jnp.minimum(jnp.sum(intersect, axis=0), CAP)
    used = slot[None, :] < counts[:, None]
    listed = jnp.einsum(
        "qsb,bqj->qsj",
        matches.astype(jnp.bfloat16),
        tiles.astype(jnp.bfloat16),
        preferred_element_type=jnp.float32,
    )
    listed = jnp.where(used[:, :, None], listed, -1.0).reshape(27, CAP * touched)
    own_tiles = tiles[:, 13, :].astype(jnp.float32).reshape(own_lists, CAP * touched)
    listed = jnp.concatenate([listed[:13], own_tiles[:1], listed[14:], own_tiles[1:]], axis=0)
    own_picks = bubble.reshape(own_lists, CAP)
    picks = jnp.concatenate([picked[:13], own_picks[:1], picked[14:], own_picks[1:]], axis=0)
    counts = jnp.concatenate(
        [counts[:13], jnp.full((1,), CAP), counts[14:], jnp.full((own_lists - 1,), CAP)]
    )
    lists = jnp.concatenate([picks.reshape(-1), counts]).astype(jnp.float32)
    lists = jnp.pad(lists, (0, -lists.shape[0] % markers)).reshape(-1, markers)
    packed = jnp.concatenate(
        [
            marker_pos.transpose(1, 0, 2).reshape(-1, markers),
            marker_force.transpose(1, 0, 2).reshape(-1, markers),
            listed,
            lists,
        ],
        axis=0,
    )
    return jnp.pad(packed, ((0, -packed.shape[0] % 8), (0, 0)))


class Sizes:
    def __init__(self, velocity, marker_pos, tiles):
        self.bubbles, _, self.markers = marker_pos.shape
        self.size_x, self.size_y, _, self.tile_len = velocity.shape
        self.touched = tiles.shape[2]
        self.tile_total = self.size_x * self.size_y
        self.width = CAP * self.touched
        assert self.width == self.markers
        self.own_lists = self.bubbles // CAP
        self.n_lists = 26 + self.own_lists
        self.list_row = 6 * self.bubbles + self.n_lists

    def meta(self, blocks):
        rows = -(-(self.n_lists * (CAP + 1)) // self.markers)
        self.meta_len = rows * self.markers
        parts = [b[self.list_row : self.list_row + rows].reshape(-1) for b in blocks]
        return jnp.concatenate(parts).astype(jnp.int32)


def stack_blocks(z, blocks, data, cell):
    cell[...] = lax.broadcasted_iota(jnp.int32, cell.shape, 0).astype(jnp.float32) * scale
    for i, block in enumerate(blocks):
        data[i] = block[...]


def batch_setup(z, tab, meta, meta_at, data, cols, i):
    src, lst = tab[6 * i], tab[6 * i + 1]
    base = (src + meta_at) * z.meta_len
    count = meta[base + z.n_lists * CAP + lst]
    tile_row = data[src, pl.ds(6 * z.bubbles + lst, 1), :]
    tile_x = jnp.floor((tile_row + 0.5) * (1.0 / z.size_y))
    tile_y = tile_row - tile_x * z.size_y
    which = lax.broadcasted_iota(jnp.int32, (8, z.width), 0)
    stacked = jnp.where(
        which == 0, tile_row, jnp.where(which == 1, tile_x * scale, tile_y * scale)
    )
    cols[...] = stacked.T
    shift_x = (tab[6 * i + 3] * z.size_x).astype(jnp.float32)
    shift_y = (tab[6 * i + 4] * z.size_y).astype(jnp.float32)
    shift_z = (tab[6 * i + 5] * z.tile_len).astype(jnp.float32)
    return src, base + lst * CAP, count, tile_row, (shift_x, shift_y, shift_z)


def row_weights(z, data, cols, cell, src, bubble, slot, shifts):
    def coordinate(k):
        return (data[src, pl.ds(k * z.bubbles + bubble, 1), :] - shifts[k]) * scale

    dz = (cell[...] - coordinate(2)).astype(jnp.bfloat16)
    along = jnp.exp2(-(dz * dz))
    mine = cols[pl.ds(slot * z.touched, z.touched), :]
    dx = jnp.broadcast_to(mine[:, 1:2], (z.touched, z.markers)) - coordinate(0)
    dy = jnp.broadcast_to(mine[:, 2:3], (z.touched, z.markers)) - coordinate(1)
    return along, jnp.exp2(-(dx * dx + dy * dy))


def spread_kernel(z, n_blocks, n_init, n_batches, meta_at, *refs):
    tab, meta = refs[:2]
    blocks = refs[2 : 2 + n_blocks]
    inits = refs[2 + n_blocks : 2 + n_blocks + n_init]
    acc, data, cols, cell, pieces = refs[2 + n_blocks + n_init :]
    stack_blocks(z, blocks, data, cell)
    if n_init:
        total = inits[0][...]
        for init in inits[1:]:
            total = total + init[...]
        acc[...] = total
    else:
        acc[...] = jnp.zeros_like(acc)
    pieces[...] = jnp.zeros_like(pieces)

    def batch(i, carry):
        src, first, count, tile_row, shifts = batch_setup(z, tab, meta, meta_at, data, cols, i)
        target = tab[6 * i + 2]

        def rows_of(n):
            for slot in range(n):
                bubble = meta[first + slot]
                along, across = row_weights(z, data, cols, cell, src, bubble, slot, shifts)
                scaled = [
                    (data[src, pl.ds((3 + k) * z.bubbles + bubble, 1), :] * across).astype(
                        jnp.bfloat16
                    )
                    for k in range(3)
                ]
                piece = lax.dot_general(
                    jnp.concatenate(scaled, axis=0),
                    along,
                    (((1,), (1,)), ((), ())),
                    preferred_element_type=jnp.float32,
                ).astype(jnp.bfloat16)
                at = pl.ds(slot * z.touched, z.touched)
                for k in range(3):
                    pieces[at, k * z.tile_len : (k + 1) * z.tile_len] = piece[
                        k * z.touched : (k + 1) * z.touched
                    ]

        least = -1
        for n in STEPS:
            pl.when((count > least) & (count <= n))(functools.partial(rows_of, n))
            least = n
        tile = lax.broadcasted_iota(jnp.int32, (z.tile_total, z.width), 0).astype(jnp.float32)
        placing = (tile == tile_row).astype(jnp.float32).astype(jnp.bfloat16)
        added = jnp.dot(placing, pieces[...], preferred_element_type=jnp.float32)
        for k in range(3):
            acc[target, k] += added[:, k * z.tile_len : (k + 1) * z.tile_len]
        return carry

    lax.fori_loop(0, n_batches, batch, 0)


def cost(z, n_batches):
    rows = n_batches * CAP
    return pl.CostEstimate(
        flops=rows * 2 * 3 * z.touched * z.markers * z.tile_len * 8,
        bytes_accessed=4 << 20,
        transcendentals=rows * z.markers * z.tile_len,
    )


def spread(z, meta, meta_at, blocks, batches, n_acc, inits, name):
    table = jnp.asarray(np.array(batches, np.int32).reshape(-1))
    return pl.pallas_call(
        functools.partial(spread_kernel, z, len(blocks), len(inits), len(batches), meta_at),
        compiler_params=pltpu.CompilerParams(vmem_limit_bytes=VMEM_LIMIT),
        out_shape=jax.ShapeDtypeStruct((n_acc, 3, z.tile_total, z.tile_len), jnp.float32),
        in_specs=[SMEM, SMEM] + [VMEM] * (len(blocks) + len(inits)),
        out_specs=VMEM,
        scratch_shapes=[
            pltpu.VMEM((len(blocks),) + blocks[0].shape, jnp.float32),
            pltpu.VMEM((z.width, 8), jnp.float32),
            pltpu.VMEM((z.tile_len, z.markers), jnp.float32),
            pltpu.VMEM((z.width, 3 * z.tile_len), jnp.bfloat16),
        ],
        cost_estimate=cost(z, len(batches)),
        name=name,
    )(table, meta, *blocks, *inits)


def sample_kernel(z, n_blocks, n_grids, n_init, n_batches, meta_at, *refs):
    tab, meta = refs[:2]
    at = 2 + n_blocks
    blocks = refs[2:at]
    grids = refs[at : at + n_grids]
    inits = refs[at + n_grids : at + n_grids + n_init]
    outs = refs[at + n_grids + n_init : at + n_grids + n_init + n_blocks]
    data, cols, cell, local, low, acc = refs[at + n_grids + n_init + n_blocks :]
    stack_blocks(z, blocks, data, cell)
    for i in range(n_blocks):
        acc[i] = inits[i][...] if n_init else jnp.zeros_like(inits[i] if n_init else outs[i])
    for i, grid in enumerate(grids):
        for k in range(3):
            low[i, :, k * z.tile_len : (k + 1) * z.tile_len] = grid[k].astype(jnp.bfloat16)

    def batch(i, carry):
        src, first, count, _, shifts = batch_setup(z, tab, meta, meta_at, data, cols, i)
        target = tab[6 * i + 2]
        tile = lax.broadcasted_iota(jnp.int32, (z.width, z.tile_total), 1).astype(jnp.float32)
        picking = (jnp.broadcast_to(cols[:, 0:1], tile.shape) == tile).astype(jnp.float32)
        local[...] = jnp.dot(
            picking.astype(jnp.bfloat16), low[target], preferred_element_type=jnp.float32
        ).astype(jnp.bfloat16)

        def rows_of(n):
            for slot in range(n):
                bubble = meta[first + slot]
                along, across = row_weights(z, data, cols, cell, src, bubble, slot, shifts)
                rows = local[pl.ds(slot * z.touched, z.touched), :]
                u = jnp.concatenate(
                    [rows[:, k * z.tile_len : (k + 1) * z.tile_len] for k in range(3)], axis=0
                )
                sampled = jnp.dot(u, along, preferred_element_type=jnp.float32)
                for k in range(3):
                    part = jnp.sum(
                        sampled[k * z.touched : (k + 1) * z.touched] * across,
                        axis=0,
                        keepdims=True,
                    )
                    acc[src, pl.ds(k * z.bubbles + bubble, 1), :] += part

        least = -1
        for n in STEPS:
            pl.when((count > least) & (count <= n))(functools.partial(rows_of, n))
            least = n
        return carry

    lax.fori_loop(0, n_batches, batch, 0)
    for i in range(n_blocks):
        outs[i][...] = acc[i]


def sample(z, meta, meta_at, blocks, grids, batches, inits, name):
    table = jnp.asarray(np.array(batches, np.int32).reshape(-1))
    n = len(blocks)
    shape = (3 * z.bubbles, z.markers)
    return pl.pallas_call(
        functools.partial(sample_kernel, z, n, len(grids), len(inits), len(batches), meta_at),
        compiler_params=pltpu.CompilerParams(vmem_limit_bytes=VMEM_LIMIT),
        out_shape=[jax.ShapeDtypeStruct(shape, jnp.float32)] * n,
        in_specs=[SMEM, SMEM] + [VMEM] * (n + len(grids) + len(inits)),
        out_specs=[VMEM] * n,
        scratch_shapes=[
            pltpu.VMEM((n,) + blocks[0].shape, jnp.float32),
            pltpu.VMEM((z.width, 8), jnp.float32),
            pltpu.VMEM((z.tile_len, z.markers), jnp.float32),
            pltpu.VMEM((z.width, 3 * z.tile_len), jnp.bfloat16),
            pltpu.VMEM((len(grids), z.tile_total, 3 * z.tile_len), jnp.bfloat16),
            pltpu.VMEM((n,) + shape, jnp.float32),
        ],
        cost_estimate=cost(z, len(batches)),
        name=name,
    )(table, meta, *blocks, *grids, *inits)


def smooth_kernel(vel, x_low, x_high, y_low, y_high, out):
    _, size_x, size_y, tile_len = vel.shape
    total = size_x * size_y
    row = lax.broadcasted_iota(jnp.int32, (size_x, size_y, tile_len), 1)
    lane = lax.broadcasted_iota(jnp.int32, (total, tile_len), 1)
    for k in range(3):
        v = vel[k]
        flat = v.reshape(total, tile_len)
        up = jnp.concatenate([x_low[k][None], v[:-1]], axis=0)
        down = jnp.concatenate([v[1:], x_high[k][None]], axis=0)
        left = jnp.where(row == 0, y_low[k][:, None, :], pltpu.roll(v, 1, 1))
        right = jnp.where(row == size_y - 1, y_high[k][:, None, :], pltpu.roll(v, size_y - 1, 1))
        before = pltpu.roll(flat, 1, 1)
        after = pltpu.roll(flat, tile_len - 1, 1)
        near = (up + down + left + right).reshape(total, tile_len)
        near = near + jnp.where(lane == 0, 0.0, before)
        near = near + jnp.where(lane == tile_len - 1, 0.0, after)
        out[0, k] = flat + viscous * (near - 6.0 * flat)
        out[1, k] = jnp.where(lane == tile_len - 1, viscous * after, 0.0)
        out[2, k] = jnp.where(lane == 0, viscous * before, 0.0)


def body(velocity, marker_pos, marker_force, intersect, tiles):
    z = Sizes(velocity, marker_pos, tiles)
    vel = velocity.transpose(2, 0, 1, 3)

    def code(ox, oy, oz):
        return 9 * (ox + 1) + 3 * (oy + 1) + oz + 1

    x_low = shifted(vel[:, -1], "gx", 1)
    x_high = shifted(vel[:, 0], "gx", -1)
    y_low = shifted(vel[:, :, -1], "gy", 1)
    y_high = shifted(vel[:, :, 0], "gy", -1)

    own = message(marker_pos, marker_force, intersect, tiles)
    own, x_low, x_high, y_low, y_high = lax.optimization_barrier(
        (own, x_low, x_high, y_low, y_high)
    )
    if lax.axis_size("gx") == 2:
        x_steps = [(1, (1, -1))]
    else:
        x_steps = [(1, (1,)), (-1, (-1,))]
    x_blocks = [shifted(own, "gx", step) for step, _ in x_steps]
    y_blocks = [shifted(own, "gy", step) for step in (1, -1)]
    xy_blocks = [shifted(block, "gy", step) for step in (1, -1) for block in x_blocks]

    order = {0: 0, -1: 1, 1: 2}

    def own_batches(zs, slot_of):
        found = []
        for oz in zs:
            if oz == 0:
                found += [(0, q, slot_of[0], 0, 0, 0) for q in [13] + list(range(27, z.n_lists))]
            else:
                found.append((0, code(0, 0, oz), slot_of[oz], 0, 0, oz))
        return found

    def x_batches(zs, slot_of, base=0):
        return [
            (base + i, code(ox, 0, oz), slot_of[oz], ox, 0, oz)
            for i, (_, oxs) in enumerate(x_steps)
            for ox in oxs
            for oz in zs
        ]

    def y_batches(zs, slot_of, base=0):
        return [
            (base + i, code(0, oy, oz), slot_of[oz], 0, oy, oz)
            for i, oy in enumerate((1, -1))
            for oz in zs
        ]

    def xy_batches(zs, slot_of, base=0):
        return [
            (base + i * len(x_steps) + j, code(ox, oy, oz), slot_of[oz], ox, oy, oz)
            for i, oy in enumerate((1, -1))
            for j, (_, oxs) in enumerate(x_steps)
            for ox in oxs
            for oz in zs
        ]

    n_x = len(x_steps)
    every, outer, zero, sides = (-1, 1, 0), (-1, 1), {0: 0}, {-1: 0, 1: 1}
    metas = [z.meta([own])]
    acc = spread(z, metas[0], 0, [own], own_batches(every, order), 3, [], "spread_own")
    smooth = pl.pallas_call(
        smooth_kernel,
        out_shape=jax.ShapeDtypeStruct((3, 3, z.tile_total, z.tile_len), jnp.float32),
        in_specs=[VMEM] * 5,
        out_specs=VMEM,
        compiler_params=pltpu.CompilerParams(vmem_limit_bytes=VMEM_LIMIT),
        name="smooth",
    )(vel, x_low, x_high, y_low, y_high)
    mid = x_blocks + y_blocks
    metas.append(z.meta(mid))
    acc = spread(
        z,
        metas[1],
        0,
        mid,
        x_batches(outer, order) + y_batches(outer, order, n_x),
        3,
        [acc, smooth],
        "spread_mid",
    )
    metas.append(z.meta(xy_blocks))
    acc = spread(
        z, metas[2], 0, xy_blocks, xy_batches(outer, order), 3, [acc], "spread_far"
    )
    from_high = shifted(acc[1], "gz", -1)
    from_low = shifted(acc[2], "gz", 1)
    near = [own] + x_blocks
    far = y_blocks + xy_blocks
    meta = jnp.concatenate(metas)
    late = x_batches((0,), zero) + y_batches((0,), zero, n_x) + xy_batches((0,), zero, n_x + 2)
    last = spread(z, meta, 1, x_blocks + far, late, 1, [acc[:1]], "spread_late")
    result = last[0] + from_high + from_low
    low_grid = shifted(result, "gz", 1)
    high_grid = shifted(result, "gz", -1)
    velocity_out = result.reshape(3, z.size_x, z.size_y, z.tile_len).transpose(1, 2, 0, 3)

    here = (
        own_batches((0,), zero)
        + x_batches((0,), zero, 1)
        + y_batches((0,), zero, 1 + n_x)
        + xy_batches((0,), zero, 3 + n_x)
    )
    part = sample(z, meta, 0, near + far, [result], here, [], "sample_here")
    far_part = sample(
        z,
        meta,
        1 + n_x,
        far,
        [low_grid, high_grid],
        y_batches(outer, sides) + xy_batches(outer, sides, 2),
        part[1 + n_x :],
        "sample_far",
    )
    xy_back = [
        shifted(far_part[2 + i * n_x + j], "gy", -oy) for i, oy in enumerate((1, -1)) for j in range(n_x)
    ]
    y_back = [shifted(far_part[i], "gy", -oy) for i, oy in enumerate((1, -1))]
    near_part = sample(
        z,
        meta,
        0,
        near,
        [low_grid, high_grid],
        own_batches(outer, sides) + x_batches(outer, sides, 1),
        part[: 1 + n_x],
        "sample_near",
    )
    total = near_part[0]
    for j, (step, _) in enumerate(x_steps):
        side = near_part[1 + j] + xy_back[j] + xy_back[n_x + j]
        total = total + shifted(side, "gx", -step)
    total = total + y_back[0] + y_back[1]
    marker_velocity = total.reshape(3, z.bubbles, z.markers).transpose(1, 0, 2)
    return (velocity_out, marker_velocity)


def solution(mesh):
    rows = P(("gx", "gy", "gz"), None, None)
    grid = P("gx", "gy", None, "gz")
    return jax.shard_map(
        body,
        mesh=mesh,
        in_specs=(grid, rows, rows, P(("gx", "gy", "gz"), None), rows),
        out_specs=(grid, rows),
        check_vma=False,
    )
```

```python
import functools

import jax
import jax.numpy as jnp
import numpy as np
from jax import lax
from jax.experimental import pallas as pl
from jax.experimental.pallas import tpu as pltpu
from jax.sharding import PartitionSpec as P

CAP = 16
STEPS = (CAP // 4, CAP // 2, CAP)
VMEM_LIMIT = 20 << 20

spread_width = 0.5
viscous = 0.1
scale = float(np.sqrt(spread_width * np.log2(np.e)))

VMEM = pl.BlockSpec(memory_space=pltpu.VMEM)
SMEM = pl.BlockSpec(memory_space=pltpu.SMEM)


def shifted(value, axis, step):
    count = lax.axis_size(axis)
    return lax.ppermute(value, axis, [(i, (i + step) % count) for i in range(count)])


def message(marker_pos, marker_force, intersect, tiles):
    bubbles, _, markers = marker_pos.shape
    touched = tiles.shape[2]
    own_lists = bubbles // CAP
    ranking = jnp.cumsum(intersect, axis=0) - 1
    slot = jnp.arange(CAP, dtype=jnp.int32)
    matches = (ranking.T[:, None, :] == slot[None, :, None]) & (intersect.T[:, None, :] == 1)
    bubble = jnp.arange(bubbles, dtype=jnp.int32)
    picked = jnp.sum(jnp.where(matches, bubble[None, None, :], 0), axis=2)
    counts = jnp.minimum(jnp.sum(intersect, axis=0), CAP)
    used = slot[None, :] < counts[:, None]
    listed = jnp.einsum(
        "qsb,bqj->qsj",
        matches.astype(jnp.bfloat16),
        tiles.astype(jnp.bfloat16),
        preferred_element_type=jnp.float32,
    )
    listed = jnp.where(used[:, :, None], listed, -1.0).reshape(27, CAP * touched)
    own_tiles = tiles[:, 13, :].astype(jnp.float32).reshape(own_lists, CAP * touched)
    listed = jnp.concatenate([listed[:13], own_tiles[:1], listed[14:], own_tiles[1:]], axis=0)
    own_picks = bubble.reshape(own_lists, CAP)
    picks = jnp.concatenate([picked[:13], own_picks[:1], picked[14:], own_picks[1:]], axis=0)
    counts = jnp.concatenate(
        [counts[:13], jnp.full((1,), CAP), counts[14:], jnp.full((own_lists - 1,), CAP)]
    )
    lists = jnp.concatenate([picks.reshape(-1), counts]).astype(jnp.float32)
    lists = jnp.pad(lists, (0, -lists.shape[0] % markers)).reshape(-1, markers)
    packed = jnp.concatenate(
        [
            marker_pos.transpose(1, 0, 2).reshape(-1, markers),
            marker_force.transpose(1, 0, 2).reshape(-1, markers),
            listed,
            lists,
        ],
        axis=0,
    )
    return jnp.pad(packed, ((0, -packed.shape[0] % 8), (0, 0)))


class Sizes:
    def __init__(self, velocity, marker_pos, tiles):
        self.bubbles, _, self.markers = marker_pos.shape
        self.size_x, self.size_y, _, self.tile_len = velocity.shape
        self.touched = tiles.shape[2]
        self.tile_total = self.size_x * self.size_y
        self.width = CAP * self.touched
        assert self.width == self.markers
        self.own_lists = self.bubbles // CAP
        self.n_lists = 26 + self.own_lists
        self.list_row = 6 * self.bubbles + self.n_lists

    def meta(self, blocks):
        rows = -(-(self.n_lists * (CAP + 1)) // self.markers)
        self.meta_len = rows * self.markers
        parts = [b[self.list_row : self.list_row + rows].reshape(-1) for b in blocks]
        return jnp.concatenate(parts).astype(jnp.int32)


def stack_blocks(z, blocks, data, cell):
    cell[...] = lax.broadcasted_iota(jnp.int32, cell.shape, 0).astype(jnp.float32) * scale
    for i, block in enumerate(blocks):
        data[i] = block[...]


def batch_setup(z, tab, meta, meta_at, data, cols, i):
    src, lst = tab[6 * i], tab[6 * i + 1]
    base = (src + meta_at) * z.meta_len
    count = meta[base + z.n_lists * CAP + lst]
    tile_row = data[src, pl.ds(6 * z.bubbles + lst, 1), :]
    tile_x = jnp.floor((tile_row + 0.5) * (1.0 / z.size_y))
    tile_y = tile_row - tile_x * z.size_y
    which = lax.broadcasted_iota(jnp.int32, (8, z.width), 0)
    stacked = jnp.where(
        which == 0, tile_row, jnp.where(which == 1, tile_x * scale, tile_y * scale)
    )
    cols[...] = stacked.T
    shift_x = (tab[6 * i + 3] * z.size_x).astype(jnp.float32)
    shift_y = (tab[6 * i + 4] * z.size_y).astype(jnp.float32)
    shift_z = (tab[6 * i + 5] * z.tile_len).astype(jnp.float32)
    return src, base + lst * CAP, count, tile_row, (shift_x, shift_y, shift_z)


def row_weights(z, data, cols, cell, src, bubble, slot, shifts):
    def coordinate(k):
        return (data[src, pl.ds(k * z.bubbles + bubble, 1), :] - shifts[k]) * scale

    dz = (cell[...] - coordinate(2)).astype(jnp.bfloat16)
    along = jnp.exp2(-(dz * dz))
    mine = cols[pl.ds(slot * z.touched, z.touched), :]
    dx = jnp.broadcast_to(mine[:, 1:2], (z.touched, z.markers)) - coordinate(0)
    dy = jnp.broadcast_to(mine[:, 2:3], (z.touched, z.markers)) - coordinate(1)
    return along, jnp.exp2(-(dx * dx + dy * dy))


def spread_kernel(z, n_blocks, n_init, n_batches, meta_at, *refs):
    tab, meta = refs[:2]
    blocks = refs[2 : 2 + n_blocks]
    inits = refs[2 + n_blocks : 2 + n_blocks + n_init]
    acc, data, cols, cell, pieces = refs[2 + n_blocks + n_init :]
    stack_blocks(z, blocks, data, cell)
    if n_init:
        total = inits[0][...]
        for init in inits[1:]:
            total = total + init[...]
        acc[...] = total
    else:
        acc[...] = jnp.zeros_like(acc)
    pieces[...] = jnp.zeros_like(pieces)

    def batch(i, carry):
        src, first, count, tile_row, shifts = batch_setup(z, tab, meta, meta_at, data, cols, i)
        target = tab[6 * i + 2]

        def rows_of(n):
            for slot in range(n):
                bubble = meta[first + slot]
                along, across = row_weights(z, data, cols, cell, src, bubble, slot, shifts)
                scaled = [
                    (data[src, pl.ds((3 + k) * z.bubbles + bubble, 1), :] * across).astype(
                        jnp.bfloat16
                    )
                    for k in range(3)
                ]
                piece = lax.dot_general(
                    jnp.concatenate(scaled, axis=0),
                    along,
                    (((1,), (1,)), ((), ())),
                    preferred_element_type=jnp.float32,
                ).astype(jnp.bfloat16)
                at = pl.ds(slot * z.touched, z.touched)
                for k in range(3):
                    pieces[at, k * z.tile_len : (k + 1) * z.tile_len] = piece[
                        k * z.touched : (k + 1) * z.touched
                    ]

        least = -1
        for n in STEPS:
            pl.when((count > least) & (count <= n))(functools.partial(rows_of, n))
            least = n
        tile = lax.broadcasted_iota(jnp.int32, (z.tile_total, z.width), 0).astype(jnp.float32)
        placing = (tile == tile_row).astype(jnp.float32).astype(jnp.bfloat16)
        added = jnp.dot(placing, pieces[...], preferred_element_type=jnp.float32)
        for k in range(3):
            acc[target, k] += added[:, k * z.tile_len : (k + 1) * z.tile_len]
        return carry

    lax.fori_loop(0, n_batches, batch, 0)


def cost(z, n_batches):
    rows = n_batches * CAP
    return pl.CostEstimate(
        flops=rows * 2 * 3 * z.touched * z.markers * z.tile_len * 8,
        bytes_accessed=4 << 20,
        transcendentals=rows * z.markers * z.tile_len,
    )


def spread(z, meta, meta_at, blocks, batches, n_acc, inits, name):
    table = jnp.asarray(np.array(batches, np.int32).reshape(-1))
    return pl.pallas_call(
        functools.partial(spread_kernel, z, len(blocks), len(inits), len(batches), meta_at),
        compiler_params=pltpu.CompilerParams(vmem_limit_bytes=VMEM_LIMIT),
        out_shape=jax.ShapeDtypeStruct((n_acc, 3, z.tile_total, z.tile_len), jnp.float32),
        in_specs=[SMEM, SMEM] + [VMEM] * (len(blocks) + len(inits)),
        out_specs=VMEM,
        scratch_shapes=[
            pltpu.VMEM((len(blocks),) + blocks[0].shape, jnp.float32),
            pltpu.VMEM((z.width, 8), jnp.float32),
            pltpu.VMEM((z.tile_len, z.markers), jnp.float32),
            pltpu.VMEM((z.width, 3 * z.tile_len), jnp.bfloat16),
        ],
        cost_estimate=cost(z, len(batches)),
        name=name,
    )(table, meta, *blocks, *inits)


def sample_kernel(z, n_blocks, n_grids, n_init, n_batches, meta_at, *refs):
    tab, meta = refs[:2]
    at = 2 + n_blocks
    blocks = refs[2:at]
    grids = refs[at : at + n_grids]
    inits = refs[at + n_grids : at + n_grids + n_init]
    outs = refs[at + n_grids + n_init : at + n_grids + n_init + n_blocks]
    data, cols, cell, local, low, acc = refs[at + n_grids + n_init + n_blocks :]
    stack_blocks(z, blocks, data, cell)
    for i in range(n_blocks):
        acc[i] = inits[i][...] if n_init else jnp.zeros_like(inits[i] if n_init else outs[i])
    for i, grid in enumerate(grids):
        for k in range(3):
            low[i, :, k * z.tile_len : (k + 1) * z.tile_len] = grid[k].astype(jnp.bfloat16)

    def batch(i, carry):
        src, first, count, _, shifts = batch_setup(z, tab, meta, meta_at, data, cols, i)
        target = tab[6 * i + 2]
        tile = lax.broadcasted_iota(jnp.int32, (z.width, z.tile_total), 1).astype(jnp.float32)
        picking = (jnp.broadcast_to(cols[:, 0:1], tile.shape) == tile).astype(jnp.float32)
        local[...] = jnp.dot(
            picking.astype(jnp.bfloat16), low[target], preferred_element_type=jnp.float32
        ).astype(jnp.bfloat16)

        def rows_of(n):
            for slot in range(n):
                bubble = meta[first + slot]
                along, across = row_weights(z, data, cols, cell, src, bubble, slot, shifts)
                rows = local[pl.ds(slot * z.touched, z.touched), :]
                u = jnp.concatenate(
                    [rows[:, k * z.tile_len : (k + 1) * z.tile_len] for k in range(3)], axis=0
                )
                sampled = jnp.dot(u, along, preferred_element_type=jnp.float32)
                for k in range(3):
                    part = jnp.sum(
                        sampled[k * z.touched : (k + 1) * z.touched] * across,
                        axis=0,
                        keepdims=True,
                    )
                    acc[src, pl.ds(k * z.bubbles + bubble, 1), :] += part

        least = -1
        for n in STEPS:
            pl.when((count > least) & (count <= n))(functools.partial(rows_of, n))
            least = n
        return carry

    lax.fori_loop(0, n_batches, batch, 0)
    for i in range(n_blocks):
        outs[i][...] = acc[i]


def sample(z, meta, meta_at, blocks, grids, batches, inits, name):
    table = jnp.asarray(np.array(batches, np.int32).reshape(-1))
    n = len(blocks)
    shape = (3 * z.bubbles, z.markers)
    return pl.pallas_call(
        functools.partial(sample_kernel, z, n, len(grids), len(inits), len(batches), meta_at),
        compiler_params=pltpu.CompilerParams(vmem_limit_bytes=VMEM_LIMIT),
        out_shape=[jax.ShapeDtypeStruct(shape, jnp.float32)] * n,
        in_specs=[SMEM, SMEM] + [VMEM] * (n + len(grids) + len(inits)),
        out_specs=[VMEM] * n,
        scratch_shapes=[
            pltpu.VMEM((n,) + blocks[0].shape, jnp.float32),
            pltpu.VMEM((z.width, 8), jnp.float32),
            pltpu.VMEM((z.tile_len, z.markers), jnp.float32),
            pltpu.VMEM((z.width, 3 * z.tile_len), jnp.bfloat16),
            pltpu.VMEM((len(grids), z.tile_total, 3 * z.tile_len), jnp.bfloat16),
            pltpu.VMEM((n,) + shape, jnp.float32),
        ],
        cost_estimate=cost(z, len(batches)),
        name=name,
    )(table, meta, *blocks, *grids, *inits)


def smooth_kernel(vel, x_low, x_high, y_low, y_high, out):
    _, size_x, size_y, tile_len = vel.shape
    total = size_x * size_y
    row = lax.broadcasted_iota(jnp.int32, (size_x, size_y, tile_len), 1)
    lane = lax.broadcasted_iota(jnp.int32, (total, tile_len), 1)
    for k in range(3):
        v = vel[k]
        flat = v.reshape(total, tile_len)
        up = jnp.concatenate([x_low[k][None], v[:-1]], axis=0)
        down = jnp.concatenate([v[1:], x_high[k][None]], axis=0)
        left = jnp.where(row == 0, y_low[k][:, None, :], pltpu.roll(v, 1, 1))
        right = jnp.where(row == size_y - 1, y_high[k][:, None, :], pltpu.roll(v, size_y - 1, 1))
        before = pltpu.roll(flat, 1, 1)
        after = pltpu.roll(flat, tile_len - 1, 1)
        near = (up + down + left + right).reshape(total, tile_len)
        near = near + jnp.where(lane == 0, 0.0, before)
        near = near + jnp.where(lane == tile_len - 1, 0.0, after)
        out[0, k] = flat + viscous * (near - 6.0 * flat)
        out[1, k] = jnp.where(lane == tile_len - 1, viscous * after, 0.0)
        out[2, k] = jnp.where(lane == 0, viscous * before, 0.0)


def body(velocity, marker_pos, marker_force, intersect, tiles):
    z = Sizes(velocity, marker_pos, tiles)
    vel = velocity.transpose(2, 0, 1, 3)

    def code(ox, oy, oz):
        return 9 * (ox + 1) + 3 * (oy + 1) + oz + 1

    x_low = shifted(vel[:, -1], "gx", 1)
    x_high = shifted(vel[:, 0], "gx", -1)
    y_low = shifted(vel[:, :, -1], "gy", 1)
    y_high = shifted(vel[:, :, 0], "gy", -1)

    own = message(marker_pos, marker_force, intersect, tiles)
    own, x_low, x_high, y_low, y_high = lax.optimization_barrier(
        (own, x_low, x_high, y_low, y_high)
    )
    if lax.axis_size("gx") == 2:
        x_steps = [(1, (1, -1))]
    else:
        x_steps = [(1, (1,)), (-1, (-1,))]
    x_blocks = [shifted(own, "gx", step) for step, _ in x_steps]
    y_blocks = [shifted(own, "gy", step) for step in (1, -1)]
    xy_blocks = [shifted(block, "gy", step) for step in (1, -1) for block in x_blocks]

    order = {0: 0, -1: 1, 1: 2}

    def own_batches(zs, slot_of):
        found = []
        for oz in zs:
            if oz == 0:
                found += [(0, q, slot_of[0], 0, 0, 0) for q in [13] + list(range(27, z.n_lists))]
            else:
                found.append((0, code(0, 0, oz), slot_of[oz], 0, 0, oz))
        return found

    def x_batches(zs, slot_of, base=0):
        return [
            (base + i, code(ox, 0, oz), slot_of[oz], ox, 0, oz)
            for i, (_, oxs) in enumerate(x_steps)
            for ox in oxs
            for oz in zs
        ]

    def y_batches(zs, slot_of, base=0):
        return [
            (base + i, code(0, oy, oz), slot_of[oz], 0, oy, oz)
            for i, oy in enumerate((1, -1))
            for oz in zs
        ]

    def xy_batches(zs, slot_of, base=0):
        return [
            (base + i * len(x_steps) + j, code(ox, oy, oz), slot_of[oz], ox, oy, oz)
            for i, oy in enumerate((1, -1))
            for j, (_, oxs) in enumerate(x_steps)
            for ox in oxs
            for oz in zs
        ]

    n_x = len(x_steps)
    every, outer, zero, sides = (-1, 1, 0), (-1, 1), {0: 0}, {-1: 0, 1: 1}
    metas = [z.meta([own])]
    acc = spread(z, metas[0], 0, [own], own_batches(every, order), 3, [], "spread_own")
    smooth = pl.pallas_call(
        smooth_kernel,
        out_shape=jax.ShapeDtypeStruct((3, 3, z.tile_total, z.tile_len), jnp.float32),
        in_specs=[VMEM] * 5,
        out_specs=VMEM,
        compiler_params=pltpu.CompilerParams(vmem_limit_bytes=VMEM_LIMIT),
        name="smooth",
    )(vel, x_low, x_high, y_low, y_high)
    mid = x_blocks + y_blocks
    metas.append(z.meta(mid))
    acc = spread(
        z,
        metas[1],
        0,
        mid,
        x_batches(outer, order) + y_batches(outer, order, n_x),
        3,
        [acc, smooth],
        "spread_mid",
    )
    metas.append(z.meta(xy_blocks))
    acc = spread(
        z, metas[2], 0, xy_blocks, xy_batches(outer, order), 3, [acc], "spread_far"
    )
    from_high = shifted(acc[1], "gz", -1)
    from_low = shifted(acc[2], "gz", 1)
    near = [own] + x_blocks
    far = y_blocks + xy_blocks
    meta = jnp.concatenate(metas)
    late = x_batches((0,), zero) + y_batches((0,), zero, n_x) + xy_batches((0,), zero, n_x + 2)
    last = spread(z, meta, 1, x_blocks + far, late, 1, [acc[:1]], "spread_late")
    result = last[0] + from_high + from_low
    low_grid = shifted(result, "gz", 1)
    high_grid = shifted(result, "gz", -1)
    velocity_out = result.reshape(3, z.size_x, z.size_y, z.tile_len).transpose(1, 2, 0, 3)

    here = (
        own_batches((0,), zero)
        + x_batches((0,), zero, 1)
        + y_batches((0,), zero, 1 + n_x)
        + xy_batches((0,), zero, 3 + n_x)
    )
    part = sample(z, meta, 0, near + far, [result], here, [], "sample_here")
    far_part = sample(
        z,
        meta,
        1 + n_x,
        far,
        [low_grid, high_grid],
        y_batches(outer, sides) + xy_batches(outer, sides, 2),
        part[1 + n_x :],
        "sample_far",
    )
    xy_back = [
        shifted(far_part[2 + i * n_x + j], "gy", -oy) for i, oy in enumerate((1, -1)) for j in range(n_x)
    ]
    y_back = [shifted(far_part[i], "gy", -oy) for i, oy in enumerate((1, -1))]
    side_part = sample(
        z,
        meta,
        1,
        x_blocks,
        [low_grid, high_grid],
        x_batches(outer, sides),
        part[1 : 1 + n_x],
        "sample_side",
    )
    own_part = sample(
        z,
        meta,
        0,
        [own],
        [low_grid, high_grid],
        own_batches(outer, sides),
        part[:1],
        "sample_own",
    )
    total = own_part[0]
    for j, (step, _) in enumerate(x_steps):
        side = side_part[j] + xy_back[j] + xy_back[n_x + j]
        total = total + shifted(side, "gx", -step)
    total = total + y_back[0] + y_back[1]
    marker_velocity = total.reshape(3, z.bubbles, z.markers).transpose(1, 0, 2)
    return (velocity_out, marker_velocity)


def solution(mesh):
    rows = P(("gx", "gy", "gz"), None, None)
    grid = P("gx", "gy", None, "gz")
    return jax.shard_map(
        body,
        mesh=mesh,
        in_specs=(grid, rows, rows, P(("gx", "gy", "gz"), None), rows),
        out_specs=(grid, rows),
        check_vma=False,
    )
```
